32 devices in a mesh: dp: 4 (over x, core), mp: 8 (over z, y).
Axes of the slice: x: 2, y: 2, z: 4, core: 2. Of those that a mesh axis runs over, the one named last changes fastest.
Arguments:
- attn_out: bfloat16 [512, 8192], P('dp', 'mp'), may hold values from -6 to 6
- residual: bfloat16 [512, 8192], P('dp', 'mp'), may hold values from -40 to 40
- output_weight: bfloat16 [8192, 8192], P('mp', 'dp'), may hold values from -0.0625 to 0.0625
- prune_mask: int32 [8192, 128], P('mp'), may hold values 0 or 1
- inverse_factor: float32 [128, 8192], P(None, 'dp'), may hold values from -2 to 2, as said below
- norm_gain: bfloat16 [8192], P('mp'), may hold values from 0.5 to 1.5
- gate_up_weight: bfloat16 [8192, 2, 14336], P('dp', None, 'mp'), may hold values from -0.0625 to 0.0625
Outputs:
- pruned_weight: bfloat16 [8192, 8192], P('mp', 'dp')
- stream: bfloat16 [512, 8192], P('dp', 'mp')
- hessian: float32 [14336, 14336], P('mp', 'dp')
The draws below stay inside these ranges and needn't reach their ends.
Inputs may be any that keep to these rules, and one draw needn't show every extreme that they name: inverse_factor is zero below its diagonal, and its diagonal lies between 0.5 and 2.
All inputs are finite; a program needn't handle non-finite values. No bound on the sum of `prune_mask` on one device may be relied on, other than what follows from the above.
Results may differ from the reference program's by a relative error of at most 0.012.
Values may be sent and summed in bfloat16 or wider, within the bound.
A program may use at most 128 MiB of HBM per device.

```python
import math
import jax
import jax.numpy as jnp
from jax import lax

D = 8192
BLK = 128
TOKENS = 512
HU = 14336


def draw_residual(key, part):
    subkeys = jax.random.split(key, 3)
    row_scale = jnp.exp(jax.random.uniform(subkeys[0], (TOKENS, 1), jnp.float32, math.log(0.3), math.log(3.0)))
    rising = 0.6 + 1.2 * jnp.arange(D, dtype=jnp.float32)[None, :] / D
    ragged = jnp.exp(jax.random.uniform(subkeys[1], (1, D), jnp.float32, math.log(0.7), math.log(1.4)))
    sample = jnp.clip(jax.random.normal(subkeys[2], (TOKENS, D), jnp.float32), -5.0, 5.0)
    return (row_scale * rising * ragged * sample).astype(jnp.bfloat16)


def draw_inverse_factor(key, part):
    subkeys = jax.random.split(key, 2)
    pivots = jnp.exp(jax.random.uniform(subkeys[0], (BLK, 1), jnp.float32, math.log(0.5), math.log(2.0)))
    spread = jnp.clip(jax.random.normal(subkeys[1], (BLK, D), jnp.float32), -4.0, 4.0)
    spread = spread / math.sqrt(BLK)
    row_index = jnp.arange(BLK)[:, None]
    col_index = jnp.arange(D)[None, :]
    shaped = jnp.where(col_index == row_index, 1.0, jnp.where(col_index > row_index, spread, 0.0))
    return (pivots * shaped).astype(jnp.float32)


def with_ends(result, key, smallest, top_value):
    extent = result.shape
    index_at = [jax.random.randint(jax.random.fold_in(key, axis), (), 0, extent[axis]) for axis in range(len(extent))]
    result = result.at[tuple(index_at)].set(smallest)
    longest = extent.index(max(extent))
    index_at[longest] = (index_at[longest] + 1) % extent[longest]
    return result.at[tuple(index_at)].set(top_value)


def steps_of(rng, dims, pieces, least, top_value):
    factor_of = 1.0
    for axis_at, blocks in pieces:
        heights = jax.random.uniform(jax.random.fold_in(jax.random.fold_in(rng, 6), axis_at), (blocks,), jnp.float32, least / len(pieces), top_value / len(pieces))
        factor_of = factor_of * jnp.repeat(jnp.exp(heights), dims[axis_at] // blocks).reshape((-1,) + (1,) * (len(dims) - 1 - axis_at))
    return factor_of


def scatter_about(rng, shape, deviation, reach, pieces=(), kind=jnp.bfloat16):
    level = steps_of(rng, shape, pieces, -0.22, 0.18) if pieces else 1.0
    values = jax.random.normal(rng, shape, jnp.float32) * deviation * level
    return jnp.minimum(jnp.maximum(values, -reach), reach).astype(kind)


def setup_inputs(seed: int = 0) -> dict:
    splits = jax.random.split(jax.random.key(seed), 8)
    return {
        "attn_out": scatter_about(splits[0], (TOKENS, D), 1.0, 6.0, ((0, 4), (1, 8))),
        "residual": draw_residual(jax.random.fold_in(splits[7], 71), 0),
        "output_weight": scatter_about(splits[2], (D, D), D ** -0.5, 0.0625, ((0, 8), (1, 4))),
        "prune_mask": with_ends((jax.random.randint(splits[3], (D, BLK), 0, 2) < 1).astype(jnp.int32), jax.random.fold_in(splits[3], 1), 0, 1),
        "inverse_factor": draw_inverse_factor(jax.random.fold_in(splits[7], 71), 0),
        "norm_gain": jnp.clip(1.0 + 0.1 * jax.random.normal(splits[5], (D,), jnp.float32), 0.5, 1.5).astype(jnp.bfloat16),
        "gate_up_weight": scatter_about(splits[6], (D, 2, HU), D ** -0.5, 0.0625, ((0, 4), (2, 8))),
    }


def reference(attn_out, residual, output_weight, prune_mask, inverse_factor, norm_gain, gate_up_weight):
    width_block = prune_mask.shape[1]
    weights = output_weight.astype(jnp.float32)
    kept_mask = prune_mask.astype(jnp.float32)

    def advance(column, errors):
        place = column.astype(jnp.int32)
        factor_column = lax.dynamic_slice_in_dim(inverse_factor, place, 1, 1)[:, 0]
        current = lax.dynamic_slice_in_dim(weights, place, 1, 1)[:, 0] - jnp.dot(errors, factor_column, precision=lax.Precision.HIGHEST)
        mask_column = lax.dynamic_slice_in_dim(kept_mask, place, 1, 1)[:, 0]
        fresh = (1.0 - mask_column) / factor_column[place] * current
        return lax.dynamic_update_slice_in_dim(errors, fresh[:, None], place, 1)
    errors = lax.fori_loop(0, width_block, advance, jnp.zeros((weights.shape[0], width_block), jnp.float32))
    updated = weights - jnp.dot(errors, inverse_factor, precision=lax.Precision.HIGHEST, preferred_element_type=jnp.float32)
    leading = updated[:, :width_block] * kept_mask
    pruned_weight = jnp.concatenate([leading, updated[:, width_block:]], axis=1).astype(jnp.bfloat16)
    projected = jnp.dot(attn_out, pruned_weight.T, preferred_element_type=jnp.float32)
    stream = (residual.astype(jnp.float32) + projected).astype(jnp.bfloat16)
    stream_float = stream.astype(jnp.float32)
    inverse = lax.rsqrt(lax.optimization_barrier(jnp.mean(stream_float * stream_float, axis=1, keepdims=True)) + 1e-05)
    normed = (stream_float * inverse * norm_gain.astype(jnp.float32)[None, :]).astype(jnp.bfloat16)
    gate_part = jnp.dot(normed, gate_up_weight[:, 0, :], preferred_element_type=jnp.float32)
    up_part = jnp.dot(normed, gate_up_weight[:, 1, :], preferred_element_type=jnp.float32)
    hidden = (jax.nn.silu(gate_part) * up_part).astype(jnp.bfloat16)
    hessian = 2.0 / hidden.shape[0] * jnp.dot(hidden.T, hidden, preferred_element_type=jnp.float32)
    return (pruned_weight, stream, hessian)
```

```python
import functools

import jax
import jax.numpy as jnp
from jax import lax
from jax.experimental import pallas as pl
from jax.experimental.pallas import tpu as pltpu
from jax.sharding import PartitionSpec as P

GROUP = 8


def from_first(block, axis):
    size, index = lax.axis_size(axis), lax.axis_index(axis)
    stride = size // 2
    while stride >= 1:
        pairs = [(i, i + stride) for i in range(0, size, 2 * stride)]
        arrived = lax.ppermute(block, axis, pairs)
        block = jnp.where(index % (2 * stride) == stride, arrived, block)
        stride //= 2
    return block


def scatter_sum(partial, axis):
    size, index = lax.axis_size(axis), lax.axis_index(axis)
    rows, cols = partial.shape
    blocks = partial.reshape(size, rows // size, cols)
    stride, left = 1, size
    while left > 1:
        halves = blocks.reshape(left // 2, 2, rows // size, cols)
        bit = (index // stride) % 2
        keep = lax.dynamic_index_in_dim(halves, bit, 1, keepdims=False)
        give = lax.dynamic_index_in_dim(halves, 1 - bit, 1, keepdims=False)
        pairs = [(i, i ^ stride) for i in range(size)]
        arrived = lax.ppermute(give.astype(jnp.bfloat16), axis, pairs)
        blocks = keep + arrived.astype(jnp.float32)
        left //= 2
        stride *= 2
    return blocks[0]


def exchange(rows_block, axis):
    size = lax.axis_size(axis)
    rows, cols = rows_block.shape
    blocks = rows_block.reshape(rows, size, cols // size).transpose(1, 0, 2)
    swapped = lax.all_to_all(blocks, axis, split_axis=0, concat_axis=0, tiled=True)
    return swapped.reshape(size * rows, cols // size)


def solve_kernel(factor_ref, weight_ref, cutting_ref, error_ref):
    count = weight_ref.shape[0] // GROUP
    error_ref[...] = weight_ref[...]

    def step(block, carry):
        base = block * GROUP
        solved = []
        for i in range(GROUP):
            value = error_ref[base + i]
            for k in range(i):
                value = value - factor_ref[base + k, base + i] * solved[k]
            solved.append(value * cutting_ref[base + i])
        for i in range(GROUP):
            error_ref[base + i] = solved[i]

        def later(other, inner):
            place = other * GROUP
            for t in range(GROUP):
                value = error_ref[place + t]
                for k in range(GROUP):
                    value = value - factor_ref[base + k, place + t] * solved[k]
                error_ref[place + t] = value
            return inner

        return lax.fori_loop(block + 1, count, later, carry)

    lax.fori_loop(0, count, step, 0)


def solve(columns, cutting, factor):
    width, rows = columns.shape
    high = 8 if rows % 1024 == 0 else 1
    shape = (width, high, rows // high)
    out = pl.pallas_call(
        solve_kernel,
        out_shape=jax.ShapeDtypeStruct(shape, jnp.float32),
        in_specs=[
            pl.BlockSpec(memory_space=pltpu.SMEM),
            pl.BlockSpec(memory_space=pltpu.VMEM),
            pl.BlockSpec(memory_space=pltpu.VMEM),
        ],
        out_specs=pl.BlockSpec(memory_space=pltpu.VMEM),
        cost_estimate=pl.CostEstimate(
            flops=width * width * rows * 8, bytes_accessed=3 * width * rows * 4, transcendentals=0
        ),
    )(factor, columns.reshape(shape), cutting.reshape(shape))
    return out.reshape(width, rows)


def body(attn_out, residual, output_weight, prune_mask, inverse_factor, norm_gain, gate_up_weight):
    width_block = prune_mask.shape[1]
    tokens, width_part = attn_out.shape
    is_first = lax.axis_index("dp") == 0

    factor = from_first(inverse_factor[:, :width_block], "dp")
    columns = from_first(output_weight[:, :width_block], "dp")
    gain_rows = jnp.broadcast_to(norm_gain[None, :], (16, width_part))
    gathered = lax.all_gather(
        jnp.concatenate([attn_out, gain_rows], axis=0), "mp", axis=1, tiled=True
    )
    gain = gathered[tokens].astype(jnp.float32)
    features = exchange(gathered[:tokens], "dp")

    pivots = jnp.diagonal(factor)
    kept = prune_mask.astype(jnp.float32)
    cutting = ((1.0 - kept) / pivots[None, :]).T
    errors = solve(columns.astype(jnp.float32).T, cutting, factor)
    updated = output_weight.astype(jnp.float32) - lax.dot_general(
        errors, inverse_factor, (((0,), (0,)), ((), ())), preferred_element_type=jnp.float32
    )
    masking = jnp.where(is_first, kept, 1.0)
    masking = jnp.pad(
        masking, ((0, 0), (0, updated.shape[1] - width_block)), constant_values=1.0
    )
    pruned_weight = (updated * masking).astype(jnp.bfloat16)

    partial = lax.dot_general(
        features, pruned_weight, (((1,), (1,)), ((), ())), preferred_element_type=jnp.float32
    )
    projected = scatter_sum(partial, "dp")
    stream = (residual.astype(jnp.float32) + projected).astype(jnp.bfloat16)

    stream_all = lax.all_gather(stream, "mp", axis=1, tiled=True).astype(jnp.float32)
    squares = jnp.sum(stream_all * stream_all, axis=1, keepdims=True)
    inverse = lax.rsqrt(squares / stream_all.shape[1] + 1e-05)
    normed = (stream_all * inverse * gain[None, :]).astype(jnp.bfloat16)
    slices = exchange(normed, "dp")

    input_rows, _, unit_count = gate_up_weight.shape
    flat_weight = gate_up_weight.reshape(input_rows, 2 * unit_count)
    gate_up = scatter_sum(
        jnp.dot(slices, flat_weight, preferred_element_type=jnp.float32), "dp"
    )
    gate_part = gate_up[:, :unit_count]
    up_part = gate_up[:, unit_count:]
    hidden = (jax.nn.silu(gate_part) * up_part).astype(jnp.bfloat16)

    window_all = lax.all_gather(hidden, "dp", axis=0, tiled=True)
    columns_all = exchange(lax.all_gather(hidden, "mp", axis=1, tiled=True), "dp")
    weighting = 2.0 / (tokens * lax.axis_size("dp"))
    hessian = weighting * lax.dot_general(
        window_all, columns_all, (((0,), (0,)), ((), ())), preferred_element_type=jnp.float32
    )
    return (pruned_weight, stream, hessian)


def solution(mesh):
    in_specs = (
        P("dp", "mp"),
        P("dp", "mp"),
        P("mp", "dp"),
        P("mp", None),
        P(None, "dp"),
        P("mp"),
        P("dp", None, "mp"),
    )
    out_specs = (P("mp", "dp"), P("dp", "mp"), P("mp", "dp"))
    return jax.shard_map(body, mesh=mesh, in_specs=in_specs, out_specs=out_specs, check_vma=False)
```
